32 devices in a mesh: seq: 8 (over y, x, core), head: 4 (over z).
Axes of the slice: x: 2, y: 2, z: 4, core: 2. Of those that a mesh axis runs over, the one named last changes fastest.
Arguments:
- tokens: bfloat16 [512, 4096], P('seq'), may hold values from -6 to 6
- norm_gain: bfloat16 [4096], replicated, may hold values from 0.25 to 1.75
- w_query: bfloat16 [4096, 4096], P(None, 'head'), may hold values from -0.09375 to 0.09375
- key_projection: bfloat16 [4096, 1024], P(None, 'head'), may hold values from -0.25 to 0.25
- value_projection: bfloat16 [4096, 1024], P(None, 'head'), may hold values from -0.09375 to 0.09375
- w_out: bfloat16 [4096, 4096], P('head'), may hold values from -0.09375 to 0.09375
- cache_keys: bfloat16 [8, 16384, 1024], P(None, 'seq', 'head'), may hold values from -60 to 60
- paged_value_cache: bfloat16 [8, 16384, 1024], P(None, 'seq', 'head'), may hold values from -6 to 6
- lengths: int32 [8], replicated, may hold values from 2048 to 16384
- parents: int32 [8, 64], replicated, may hold values from -1 to 62, as said below
- slot_block: int32 [8, 128], P(None, 'seq'), may hold values from 0 to 127, each once within a row
Outputs:
- mixed: bfloat16 [512, 4096], P('seq', 'head')
The draws below stay inside these ranges and needn't reach their ends.
Inputs may be any that keep to these rules, and one draw needn't show every extreme that they name: parents[r, 0] = -1 for the root; for j >= 1, 0 <= parents[r, j] < j; the last token's parent is always token 62. Each row of slot_block is a permutation of 0 to 127.
All inputs are finite; a program needn't handle non-finite values.
Results may differ from the reference program's by a relative error of at most 0.0054.
The reference program's roundings to bfloat16 on the way count: a program that leaves them out, or rounds other values in their place, can miss the bound.
Values may be sent and summed in bfloat16 or wider, within the bound.
A program may use at most 128 MiB of HBM per device.

```python
import jax
import jax.numpy as jnp
from jax import lax

MODEL_WIDTH = 4096
HQ = 32
KEY_VALUE_HEADS = 8
HEAD_WIDTH = 128
TQ = 64
BLK = 128
REQUEST_COUNT = 8
CTX_DEV = 2048
CONTEXT_SLOTS = 16384
NBLK = 128
TOKENS = 512
N_SEQ = 8


def draw_parents(key, part):
    node_ids = jnp.arange(TQ, dtype=jnp.int32)
    raw_bits = jax.random.randint(key, (REQUEST_COUNT, TQ), 0, 1 << 20, dtype=jnp.int32)
    picked = raw_bits % jnp.maximum(node_ids, 1)[None, :]
    picked = jnp.where(node_ids[None, :] == TQ - 1, TQ - 2, picked)
    picked = jnp.where(node_ids[None, :] == 0, -1, picked)
    return picked.astype(jnp.int32)


def draw_cache_keys(key, part):
    complete_shape = (REQUEST_COUNT, CONTEXT_SLOTS, KEY_VALUE_HEADS * HEAD_WIDTH)
    drawn = 3.0 * jax.random.truncated_normal(key, -5.0, 5.0, complete_shape, jnp.float32)
    return drawn.astype(jnp.bfloat16)


def with_ends(array, rng, low, top_value):
    dims = array.shape
    index_at = [jax.random.randint(jax.random.fold_in(rng, axis), (), 0, dims[axis]) for axis in range(len(dims))]
    array = array.at[tuple(index_at)].set(low)
    longest = dims.index(max(dims))
    index_at[longest] = (index_at[longest] + 1) % dims[longest]
    return array.at[tuple(index_at)].set(top_value)


def steps_of(rng, extent, shards, least, high):
    loudness, own = 1.0, jax.random.fold_in(rng, 6)
    for dim, parts in shards:
        heights = jnp.exp(jax.random.uniform(jax.random.fold_in(own, dim), (parts,), jnp.float32, least / len(shards), high / len(shards)))
        loudness = loudness * jnp.repeat(heights, extent[dim] // parts).reshape([-1 if axis == dim else 1 for axis in range(len(extent))])
    return loudness


def noise(rng, dims, width, reach, cuts=(), held_as=jnp.bfloat16):
    entries = jax.random.normal(rng, dims, jnp.float32) * width
    if len(cuts) > 0:
        entries = steps_of(rng, dims, cuts, -0.22, 0.18) * entries
    return jnp.clip(entries, min=-reach, max=reach).astype(held_as)


def setup_inputs(seed: int = 0) -> dict:
    seeds = jax.random.split(jax.random.key(seed), 12)
    return {
        "tokens": noise(seeds[0], (TOKENS, MODEL_WIDTH), 1.0, 6.0, ((0, 8),)),
        "norm_gain": jnp.clip(1.0 + 0.15 * jax.random.normal(seeds[1], (MODEL_WIDTH,), jnp.float32), 0.25, 1.75).astype(jnp.bfloat16),
        "w_query": noise(seeds[2], (MODEL_WIDTH, HQ * HEAD_WIDTH), MODEL_WIDTH ** -0.5, 0.09375, ((1, 4),)),
        "key_projection": noise(seeds[3], (MODEL_WIDTH, KEY_VALUE_HEADS * HEAD_WIDTH), (MODEL_WIDTH // 9) ** -0.5, 0.25, ((1, 4),)),
        "value_projection": noise(seeds[4], (MODEL_WIDTH, KEY_VALUE_HEADS * HEAD_WIDTH), MODEL_WIDTH ** -0.5, 0.09375, ((1, 4),)),
        "w_out": noise(seeds[5], (HQ * HEAD_WIDTH, MODEL_WIDTH), (HQ * HEAD_WIDTH) ** -0.5, 0.09375, ((0, 4),)),
        "cache_keys": draw_cache_keys(jax.random.fold_in(seeds[11], 71), 0),
        "paged_value_cache": noise(seeds[7], (REQUEST_COUNT, CONTEXT_SLOTS, KEY_VALUE_HEADS * HEAD_WIDTH), 1.0, 6.0, ((1, 8), (2, 4))),
        "lengths": with_ends(jax.random.randint(seeds[8], (REQUEST_COUNT,), CONTEXT_SLOTS // 8, CONTEXT_SLOTS + 1), jax.random.fold_in(seeds[8], 1), CONTEXT_SLOTS // 8, CONTEXT_SLOTS).astype(jnp.int32),
        "parents": draw_parents(jax.random.fold_in(seeds[11], 71), 0),
        "slot_block": jax.vmap(lambda own: jax.random.permutation(own, NBLK))(jax.random.split(seeds[10], REQUEST_COUNT)).reshape((REQUEST_COUNT, NBLK)).astype(jnp.int32),
    }


norm_epsilon = 1e-05
masked_score = -1e+30

def ancestors(parents):
    width_tree = parents.shape[-1]
    node_ids = jnp.arange(width_tree, dtype=jnp.int32)
    reached = (parents[..., :, None] == node_ids).astype(jnp.float32)
    reached = reached + (node_ids[:, None] == node_ids[None, :]).astype(jnp.float32)
    for repeat_step in range(max(1, (width_tree - 1).bit_length())):
        reached = jnp.minimum(jnp.einsum('rij,rjk->rik', reached, reached, precision=lax.Precision.HIGHEST), 1.0)
    return reached

def finish_group(group_max, group_total, group_sum):
    floored = jnp.maximum(group_total, 1.0)
    output = lax.optimization_barrier((group_sum / floored[..., None]).astype(jnp.bfloat16)).astype(jnp.float32)
    return (output, group_max + jnp.log(floored))

def reference(tokens, norm_gain, w_query, key_projection, value_projection, w_out, cache_keys, paged_value_cache, lengths, parents, slot_block):
    inputs = tokens.astype(jnp.float32)
    normed = (inputs * lax.rsqrt(lax.optimization_barrier(jnp.mean(inputs * inputs, axis=-1, keepdims=True)) + norm_epsilon) * norm_gain.astype(jnp.float32)).astype(jnp.bfloat16)
    queries = jnp.dot(normed, w_query, preferred_element_type=jnp.float32).astype(jnp.bfloat16)
    key_new = jnp.dot(normed, key_projection, preferred_element_type=jnp.float32).astype(jnp.bfloat16)
    value_new = jnp.dot(normed, value_projection, preferred_element_type=jnp.float32).astype(jnp.bfloat16)
    kv_heads = key_projection.shape[1] // HEAD_WIDTH
    groups = w_query.shape[1] // key_projection.shape[1]
    context = cache_keys.shape[1]
    requests = lengths.shape[0]
    score_scale = HEAD_WIDTH ** (-0.5)
    tree_mask = ancestors(parents) > 0.5
    block_offsets = jnp.arange(BLK, dtype=jnp.int32)
    positions = (slot_block[:, :, None] * BLK + block_offsets[None, None, :]).reshape(requests, context)
    visible = positions < lengths[:, None]

    def one_request(packed):
        query_rows, key_rows, value_rows, key_tree, value_tree, seen, tree_seen = packed
        query32 = query_rows.astype(jnp.float32)
        key32 = key_rows.astype(jnp.float32).reshape(N_SEQ, CTX_DEV, kv_heads, HEAD_WIDTH)
        value32 = value_rows.astype(jnp.float32).reshape(N_SEQ, CTX_DEV, kv_heads, HEAD_WIDTH)
        scores = jnp.einsum('thgd,nchd->thgnc', query32, key32, precision=lax.Precision.HIGHEST) * score_scale
        seen_groups = seen.reshape(N_SEQ, CTX_DEV)
        scores = jnp.where(seen_groups, scores, masked_score)
        group_max = scores.max(-1)
        weights = jnp.where(seen_groups, jnp.exp(scores - group_max[..., None]), 0.0)
        group_total = weights.sum(-1)
        rounded = lax.optimization_barrier(weights.astype(jnp.bfloat16)).astype(jnp.float32)
        group_sum = jnp.einsum('thgnc,nchd->thgnd', rounded, value32, precision=lax.Precision.HIGHEST)
        group_out, group_lse = finish_group(group_max, group_total, group_sum)
        tree_scores = jnp.einsum('thgd,uhd->thgu', query32, key_tree.astype(jnp.float32), precision=lax.Precision.HIGHEST) * score_scale
        tree_visible = tree_seen[:, None, None, :]
        tree_scores = jnp.where(tree_visible, tree_scores, masked_score)
        tree_max = tree_scores.max(-1)
        tree_weights = jnp.where(tree_visible, jnp.exp(tree_scores - tree_max[..., None]), 0.0)
        tree_total = tree_weights.sum(-1)
        tree_rounded = lax.optimization_barrier(tree_weights.astype(jnp.bfloat16)).astype(jnp.float32)
        tree_sum = jnp.einsum('thgu,uhd->thgd', tree_rounded, value_tree.astype(jnp.float32), precision=lax.Precision.HIGHEST)
        tree_out, tree_lse = finish_group(tree_max, tree_total, tree_sum)
        best = jnp.maximum(group_lse.max(-1), tree_lse)
        group_factor = jnp.exp(group_lse - best[..., None])
        tree_factor = jnp.exp(tree_lse - best)
        numerator = (group_out * group_factor[..., None]).sum(-2) + tree_out * tree_factor[..., None]
        total = group_factor.sum(-1) + tree_factor
        attended = (numerator / total[..., None]).astype(jnp.bfloat16)
        return attended.reshape(attended.shape[0], -1)
    packed = (queries.reshape(requests, TQ, kv_heads, groups, HEAD_WIDTH), cache_keys, paged_value_cache, key_new.reshape(requests, TQ, kv_heads, HEAD_WIDTH), value_new.reshape(requests, TQ, kv_heads, HEAD_WIDTH), visible, tree_mask)
    attended = lax.map(one_request, packed).reshape(requests * TQ, -1)
    mixed = inputs + jnp.dot(attended, w_out, preferred_element_type=jnp.float32)
    return mixed.astype(jnp.bfloat16)
```

```python
import functools

import jax
import jax.numpy as jnp
from jax import lax
from jax.experimental import pallas as pl
from jax.experimental.pallas import tpu as pltpu
from jax.sharding import PartitionSpec as P

HEAD_WIDTH = 128
TQ = 64
BLK = 128

norm_epsilon = 1e-05
masked_score = -1e30
MESH = pl.DeviceIdType.MESH
f32 = jnp.float32
bf16 = jnp.bfloat16


def xor(a, b, count):
    out, bit = 0, 1
    while bit < count:
        p, q = (a // bit) % 2, (b // bit) % 2
        out = out + bit * (p + q - 2 * p * q)
        bit *= 2
    return out


def columns_to_rows(cols, pad_rows):
    n = cols[0].shape[0]
    lane = lax.broadcasted_iota(jnp.int32, (n, 128), 1)
    tile = jnp.zeros((n, 128), f32)
    for index, col in enumerate(cols):
        tile = jnp.where(lane == index, col, tile)
    if n < 128:
        tile = jnp.concatenate([tile, jnp.zeros((128 - n, 128), f32)], axis=0)
    return tile.T[:pad_rows]


def kernel(
    dims,
    len_ref,
    slot_ref,
    parents_ref,
    gain_ref,
    tok_hbm,
    wq_hbm,
    wk_hbm,
    wv_hbm,
    wo_hbm,
    k_hbm,
    v_hbm,
    out_ref,
    tok,
    wq,
    wkv,
    wo,
    kbuf,
    vbuf,
    q_all,
    kv_own,
    reach_ref,
    bias,
    osend,
    orecv,
    lsend,
    lrecv,
    tree_out,
    att,
    zsend,
    zrecv,
    tok_sem,
    wq_sem,
    wkv_sem,
    wo_sem,
    k_sem,
    v_sem,
    q_send,
    q_recv,
    f_send,
    o_send,
    o_recv,
    l_send,
    l_recv,
    t_send,
    t_recv,
    z_send,
    z_recv,
):
    S, H, R, LR, KVH, G, LC = dims
    D = HEAD_WIDTH
    GD = G * D
    HG = KVH * G
    HGP = lsend.shape[1]
    nch = S // 2
    group = TQ // LR
    scale = D**-0.5
    exp2_scale = scale * 1.4426950408889634
    me = lax.axis_index("seq")
    mh = lax.axis_index("head")
    chip, core = me // 2, me % 2
    partner = chip * 2 + (1 - core)
    W = out_ref.shape[1]

    def remote(src, dst, ssem, rsem, seq=None, head=None):
        return pltpu.make_async_remote_copy(
            src_ref=src,
            dst_ref=dst,
            send_sem=ssem,
            recv_sem=rsem,
            device_id=(me if seq is None else seq, mh if head is None else head),
            device_id_type=MESH,
        )

    def device_at(i):
        same = xor(chip, i - 1, nch) * 2 + core
        other = xor(chip, 2 * nch - i, nch) * 2 + (1 - core)
        dev = jnp.where(i <= nch, same, other)
        dev = jnp.where(i == 1, partner, dev)
        return jnp.where(i == 0, me, dev)

    tok_copy = pltpu.make_async_copy(tok_hbm, tok, tok_sem)
    tok_copy.start()
    wq_copies = []
    for c in range(KVH):
        wq_copies.append(
            pltpu.make_async_copy(wq_hbm.at[:, c * GD : (c + 1) * GD], wq.at[c], wq_sem.at[c])
        )
        wq_copies[-1].start()
    wkv_copies = [
        pltpu.make_async_copy(wk_hbm, wkv.at[0], wkv_sem.at[0]),
        pltpu.make_async_copy(wv_hbm, wkv.at[1], wkv_sem.at[1]),
    ]
    for copy in wkv_copies:
        copy.start()

    barrier = pltpu.get_barrier_semaphore()
    for j in range(1, S):
        pl.semaphore_signal(barrier, inc=1, device_id=((me + j) % S, mh), device_id_type=MESH)
    for j in range(1, H):
        pl.semaphore_signal(barrier, inc=1, device_id=(me, (mh + j) % H), device_id_type=MESH)

    row_ids = lax.broadcasted_iota(jnp.int32, (TQ, TQ), 0)
    col_ids = lax.broadcasted_iota(jnp.int32, (TQ, TQ), 1)
    eye = row_ids == col_ids
    own_request = me // group
    parents_row = parents_ref[pl.ds(own_request, 1), :].astype(f32)
    parent_col = jnp.sum(jnp.where(eye, parents_row, 0.0), axis=1, keepdims=True)
    reached = ((parent_col == col_ids.astype(f32)) | eye).astype(f32)
    for _ in range(max(1, (TQ - 1).bit_length())):
        step = reached.astype(bf16)
        reached = jnp.minimum(jnp.dot(step, step, preferred_element_type=f32), 1.0)
    reach_ref[...] = reached

    lane = lax.broadcasted_iota(jnp.int32, (1, BLK), 1)
    for r in range(R):
        for b in range(LC // BLK):
            shown = slot_ref[r, b] * BLK + lane < len_ref[r]
            bias[r, :, b * BLK : (b + 1) * BLK] = jnp.where(shown, 0.0, masked_score)

    tok_copy.wait()
    inputs = tok[...].astype(f32)
    normed = (
        inputs
        * lax.rsqrt(jnp.mean(inputs * inputs, axis=-1, keepdims=True) + norm_epsilon)
        * gain_ref[...].astype(f32)
    ).astype(bf16)

    for c in range(KVH):
        wq_copies[c].wait()
        q_all[me, c] = jnp.dot(normed, wq[c], preferred_element_type=f32).astype(bf16)
        if c == 0:
            def load(i, carry):
                r = device_at(i) if group == 1 else i
                pltpu.make_async_copy(k_hbm.at[r], kbuf.at[r], k_sem.at[r]).start()
                pltpu.make_async_copy(v_hbm.at[r], vbuf.at[r], v_sem.at[r]).start()
                return carry

            lax.fori_loop(0, R, load, 0)
            for h in range(H):
                pltpu.make_async_copy(
                    wo_hbm.at[:, h * W : (h + 1) * W], wo.at[h], wo_sem.at[h]
                ).start()

    pl.semaphore_wait(barrier, S - 1 + H - 1)
    q_copies = []
    for i in range(1, nch + 1):
        to = partner if i == 1 else xor(chip, i - 1, nch) * 2 + core
        q_copies.append(
            remote(q_all.at[me], q_all.at[me], q_send.at[i], q_recv.at[me], seq=to)
        )
        q_copies[-1].start()

    slot = me % group
    for which in range(2):
        wkv_copies[which].wait()
        kv_own[slot, which] = jnp.dot(normed, wkv[which], preferred_element_type=f32).astype(bf16)
    base = own_request * group
    kv_copies = []
    for j in range(1, group):
        kv_copies.append(
            remote(
                kv_own.at[slot],
                kv_own.at[slot],
                t_send.at[j],
                t_recv.at[slot],
                seq=base + (slot + j) % group,
            )
        )
        kv_copies[-1].start()
    for j in range(1, group):
        source = (slot + j) % group
        remote(kv_own.at[source], kv_own.at[source], t_send.at[j], t_recv.at[source]).wait_recv()
    for copy in kv_copies:
        copy.wait_send()

    def stacked(block):
        return jnp.concatenate([block[:, g * D : (g + 1) * D] for g in range(G)], axis=0)

    seen = reach_ref[pl.ds(pl.multiple_of(slot * LR, LR), LR), :] > 0.5
    tree_cols = []
    for h in range(KVH):
        keys = jnp.concatenate([kv_own[s, 0, :, h * D : (h + 1) * D] for s in range(group)], axis=0)
        vals = jnp.concatenate([kv_own[s, 1, :, h * D : (h + 1) * D] for s in range(group)], axis=0)
        for g in range(G):
            q = q_all[me, h, :, g * D : (g + 1) * D]
            s = lax.dot_general(q, keys, (((1,), (1,)), ((), ())), preferred_element_type=f32)
            s = jnp.where(seen, s * scale, masked_score)
            m = jnp.max(s, axis=-1, keepdims=True)
            p = jnp.where(seen, jnp.exp(s - m), 0.0)
            total = jnp.maximum(jnp.sum(p, axis=-1, keepdims=True), 1.0)
            o = jnp.dot(p.astype(bf16), vals, preferred_element_type=f32)
            at = (h * G + g) * D
            tree_out[:, at : at + D] = (o / total).astype(bf16)
            tree_cols.append(m + jnp.log(total))
    tree_lse = columns_to_rows(tree_cols, HGP)

    if group > 1:
        for r in range(R):
            pltpu.make_async_copy(k_hbm.at[r], kbuf.at[r], k_sem.at[r]).wait()
            pltpu.make_async_copy(v_hbm.at[r], vbuf.at[r], v_sem.at[r]).wait()

    def attend(i, carry):
        dev = device_at(i)
        r = dev // group

        @pl.when(i > 0)
        def _():
            remote(q_all.at[dev], q_all.at[dev], q_send.at[0], q_recv.at[dev]).wait_recv()

        @pl.when((i > 1) & (i <= nch))
        def _():
            remote(
                q_all.at[dev], q_all.at[dev], f_send.at[i], q_recv.at[dev], seq=partner
            ).start()

        if group == 1:
            pltpu.make_async_copy(k_hbm.at[r], kbuf.at[r], k_sem.at[r]).wait()
            pltpu.make_async_copy(v_hbm.at[r], vbuf.at[r], v_sem.at[r]).wait()
        hidden = bias[r]
        cols = []
        for h in range(KVH):
            q = stacked(q_all[dev, h])
            keys = kbuf[r, :, h * D : (h + 1) * D]
            vals = vbuf[r, :, h * D : (h + 1) * D]
            s = lax.dot_general(q, keys, (((1,), (1,)), ((), ())), preferred_element_type=f32)
            s = s + hidden
            m = jnp.max(s, axis=-1, keepdims=True)
            p = jnp.exp2((s - m) * exp2_scale)
            total = jnp.maximum(jnp.sum(p, axis=-1, keepdims=True), 1.0)
            o = jnp.dot(p.astype(bf16), vals, preferred_element_type=f32)
            o = (o / total).astype(bf16)
            lse = m * scale + jnp.log(total)
            for g in range(G):
                at = (h * G + g) * D
                osend[dev, :, at : at + D] = o[g * LR : (g + 1) * LR]
                cols.append(lse[g * LR : (g + 1) * LR])
        lsend[dev] = columns_to_rows(cols, HGP)

        @pl.when(i > 0)
        def _():
            remote(osend.at[dev], orecv.at[me], o_send.at[i], o_recv.at[me], seq=dev).start()
            remote(lsend.at[dev], lrecv.at[me], l_send.at[i], l_recv.at[me], seq=dev).start()

        return carry

    lax.fori_loop(0, S, attend, 0)

    for copy in q_copies:
        copy.wait_send()
    for i in range(2, nch + 1):
        remote(q_all.at[me], q_all.at[me], f_send.at[i], q_recv.at[me]).wait_send()
    orecv[me] = osend[me]
    lrecv[me] = lsend[me]

    def arrive(i, carry):
        dev = device_at(i)
        remote(osend.at[dev], orecv.at[dev], o_send.at[i], o_recv.at[dev]).wait()
        remote(lsend.at[dev], lrecv.at[dev], l_send.at[i], l_recv.at[dev]).wait()
        return carry

    lax.fori_loop(1, S, arrive, 0)

    lse = [lrecv[s] for s in range(S)] + [tree_lse]
    best = functools.reduce(jnp.maximum, lse)
    factors = [jnp.exp(x - best) for x in lse]
    whole = functools.reduce(jnp.add, factors)
    rows = jnp.concatenate([x / whole for x in factors], axis=0)
    pad = -rows.shape[0] % 128
    if pad:
        rows = jnp.concatenate([rows, jnp.zeros((pad, 128), f32)], axis=0)
    weights = rows.T[:LR]
    for n in range(HG):
        at = n * D
        col = S * HGP + n
        total = weights[:, col : col + 1] * tree_out[:, at : at + D].astype(f32)
        for s in range(S):
            col = s * HGP + n
            total = total + weights[:, col : col + 1] * orecv[s, :, at : at + D].astype(f32)
        att[:, at : at + D] = total.astype(bf16)

    for h in range(H):
        pltpu.make_async_copy(wo_hbm.at[:, h * W : (h + 1) * W], wo.at[h], wo_sem.at[h]).wait()
    attended = att[...]
    order = sorted(range(1, H), key=lambda j: -min(j, H - j))
    z_copies = []
    for j in order:
        to = (mh + j) % H
        zsend[j] = jnp.dot(attended, wo[to], preferred_element_type=f32).astype(bf16)
        z_copies.append(
            remote(zsend.at[j], zrecv.at[mh], z_send.at[j], z_recv.at[mh], head=to)
        )
        z_copies[-1].start()
    mixed = jnp.dot(attended, wo[mh], preferred_element_type=f32)
    mixed = mixed + tok[:, pl.ds(pl.multiple_of(mh * W, W), W)].astype(f32)
    for j in order:
        source = (mh + H - j) % H
        remote(zsend.at[j], zrecv.at[source], z_send.at[j], z_recv.at[source]).wait_recv()
        mixed = mixed + zrecv[source].astype(f32)
    out_ref[...] = mixed.astype(bf16)
    for copy in z_copies:
        copy.wait_send()


def solution(mesh):
    S, H = mesh.shape["seq"], mesh.shape["head"]

    def per_device(
        tokens, norm_gain, w_query, key_projection, value_projection, w_out,
        cache_keys, paged_value_cache, lengths, parents, slot_block,
    ):
        LR, M = tokens.shape
        D = HEAD_WIDTH
        KVH = key_projection.shape[1] // D
        G = w_query.shape[1] // key_projection.shape[1]
        R, LC = cache_keys.shape[:2]
        W = w_out.shape[1] // H
        HG = KVH * G
        HGP = -(-HG // 8) * 8
        group = TQ // LR
        dma = pltpu.SemaphoreType.DMA
        vmem = pl.BlockSpec(memory_space=pltpu.VMEM)
        smem = pl.BlockSpec(memory_space=pltpu.SMEM)
        hbm = pl.BlockSpec(memory_space=pl.ANY)
        return pl.pallas_call(
            functools.partial(kernel, (S, H, R, LR, KVH, G, LC)),
            out_shape=jax.ShapeDtypeStruct((LR, W), bf16),
            in_specs=[smem, smem, vmem, vmem] + [hbm] * 7,
            out_specs=vmem,
            scratch_shapes=[
                pltpu.VMEM((LR, M), bf16),
                pltpu.VMEM((KVH, M, G * D), bf16),
                pltpu.VMEM((2, M, KVH * D), bf16),
                pltpu.VMEM((H, HG * D, W), bf16),
                pltpu.VMEM((R, LC, KVH * D), bf16),
                pltpu.VMEM((R, LC, KVH * D), bf16),
                pltpu.VMEM((S, KVH, LR, G * D), bf16),
                pltpu.VMEM((group, 2, LR, KVH * D), bf16),
                pltpu.VMEM((TQ, TQ), f32),
                pltpu.VMEM((R, 1, LC), f32),
                pltpu.VMEM((S, LR, HG * D), bf16),
                pltpu.VMEM((S, LR, HG * D), bf16),
                pltpu.VMEM((S, HGP, 128), f32),
                pltpu.VMEM((S, HGP, 128), f32),
                pltpu.VMEM((LR, HG * D), bf16),
                pltpu.VMEM((LR, HG * D), bf16),
                pltpu.VMEM((H, LR, W), bf16),
                pltpu.VMEM((H, LR, W), bf16),
                dma,
                dma((KVH,)),
                dma((2,)),
                dma((H,)),
                dma((R,)),
                dma((R,)),
                dma((S,)),
                dma((S,)),
                dma((S,)),
                dma((S,)),
                dma((S,)),
                dma((S,)),
                dma((S,)),
                dma((group,)),
                dma((group,)),
                dma((H,)),
                dma((H,)),
            ],
            compiler_params=pltpu.CompilerParams(
                collective_id=0, has_side_effects=True, vmem_limit_bytes=66 * 1000 * 1000
            ),
        )(
            lengths, slot_block, parents, norm_gain.reshape(1, M), tokens,
            w_query, key_projection, value_projection, w_out, cache_keys, paged_value_cache,
        )

    in_specs = (
        P("seq", None),
        P(),
        P(None, "head"),
        P(None, "head"),
        P(None, "head"),
        P("head", None),
        P(None, "seq", "head"),
        P(None, "seq", "head"),
        P(),
        P(),
        P(None, "seq"),
    )
    return jax.shard_map(
        per_device, mesh=mesh, in_specs=in_specs, out_specs=P("seq", "head"), check_vma=False
    )
```

```python
import functools

import jax
import jax.numpy as jnp
from jax import lax
from jax.experimental import pallas as pl
from jax.experimental.pallas import tpu as pltpu
from jax.sharding import PartitionSpec as P

HEAD_WIDTH = 128
TQ = 64
BLK = 128
KEYS_AT_ONCE = 512

norm_epsilon = 1e-05
masked_score = -1e30
MESH = pl.DeviceIdType.MESH
f32 = jnp.float32
bf16 = jnp.bfloat16


def xor(a, b, count):
    out, bit = 0, 1
    while bit < count:
        p, q = (a // bit) % 2, (b // bit) % 2
        out = out + bit * (p + q - 2 * p * q)
        bit *= 2
    return out


def columns_to_rows(cols, pad_rows):
    n = cols[0].shape[0]
    lane = lax.broadcasted_iota(jnp.int32, (n, 128), 1)
    tile = jnp.zeros((n, 128), f32)
    for index, col in enumerate(cols):
        tile = jnp.where(lane == index, col, tile)
    if n < 128:
        tile = jnp.concatenate([tile, jnp.zeros((128 - n, 128), f32)], axis=0)
    return tile.T[:pad_rows]


def kernel(
    dims,
    len_ref,
    slot_ref,
    parents_ref,
    gain_ref,
    tok_hbm,
    wq_hbm,
    wk_hbm,
    wv_hbm,
    wo_hbm,
    k_hbm,
    v_hbm,
    out_ref,
    tok,
    wq,
    wkv,
    wo,
    kbuf,
    vbuf,
    q_all,
    kv_own,
    reach_ref,
    bias,
    osend,
    orecv,
    lsend,
    lrecv,
    tree_out,
    att,
    zsend,
    zrecv,
    tok_sem,
    wq_sem,
    wkv_sem,
    wo_sem,
    k_sem,
    v_sem,
    q_send,
    q_recv,
    f_send,
    o_send,
    o_recv,
    l_send,
    l_recv,
    t_send,
    t_recv,
    z_send,
    z_recv,
):
    S, H, R, LR, KVH, G, LC = dims
    D = HEAD_WIDTH
    GD = G * D
    HG = KVH * G
    HGP = lsend.shape[1]
    nch = S // 2
    group = TQ // LR
    scale = D**-0.5
    exp2_scale = scale * 1.4426950408889634
    me = lax.axis_index("seq")
    mh = lax.axis_index("head")
    chip, core = me // 2, me % 2
    partner = chip * 2 + (1 - core)
    W = out_ref.shape[1]

    def remote(src, dst, ssem, rsem, seq=None, head=None):
        return pltpu.make_async_remote_copy(
            src_ref=src,
            dst_ref=dst,
            send_sem=ssem,
            recv_sem=rsem,
            device_id=(me if seq is None else seq, mh if head is None else head),
            device_id_type=MESH,
        )

    def device_at(i):
        same = xor(chip, i, nch) * 2 + core
        other = xor(chip, 2 * nch - 1 - i, nch) * 2 + (1 - core)
        return jnp.where(i < nch, same, other)

    tok_copy = pltpu.make_async_copy(tok_hbm, tok, tok_sem)
    tok_copy.start()
    wq_copies = []
    for c in range(KVH):
        wq_copies.append(
            pltpu.make_async_copy(wq_hbm.at[:, c * GD : (c + 1) * GD], wq.at[c], wq_sem.at[c])
        )
        wq_copies[-1].start()
    wkv_copies = [
        pltpu.make_async_copy(wk_hbm, wkv.at[0], wkv_sem.at[0]),
        pltpu.make_async_copy(wv_hbm, wkv.at[1], wkv_sem.at[1]),
    ]
    for copy in wkv_copies:
        copy.start()

    barrier = pltpu.get_barrier_semaphore()
    for j in range(1, S):
        pl.semaphore_signal(barrier, inc=1, device_id=((me + j) % S, mh), device_id_type=MESH)
    for j in range(1, H):
        pl.semaphore_signal(barrier, inc=1, device_id=(me, (mh + j) % H), device_id_type=MESH)

    row_ids = lax.broadcasted_iota(jnp.int32, (TQ, TQ), 0)
    col_ids = lax.broadcasted_iota(jnp.int32, (TQ, TQ), 1)
    eye = row_ids == col_ids
    own_request = me // group
    parents_row = parents_ref[pl.ds(own_request, 1), :].astype(f32)
    parent_col = jnp.sum(jnp.where(eye, parents_row, 0.0), axis=1, keepdims=True)
    reached = ((parent_col == col_ids.astype(f32)) | eye).astype(f32)
    for _ in range(max(1, (TQ - 1).bit_length())):
        step = reached.astype(bf16)
        reached = jnp.minimum(jnp.dot(step, step, preferred_element_type=f32), 1.0)
    reach_ref[...] = reached

    lane = lax.broadcasted_iota(jnp.int32, (1, BLK), 1)
    for r in range(R):
        for b in range(LC // BLK):
            shown = slot_ref[r, b] * BLK + lane < len_ref[r]
            bias[r, :, b * BLK : (b + 1) * BLK] = jnp.where(shown, 0.0, masked_score)

    tok_copy.wait()
    inputs = tok[...].astype(f32)
    normed = (
        inputs
        * lax.rsqrt(jnp.mean(inputs * inputs, axis=-1, keepdims=True) + norm_epsilon)
        * gain_ref[...].astype(f32).reshape(1, -1)
    ).astype(bf16)

    q_copies = []
    for c in range(KVH):
        wq_copies[c].wait()
        q_all[me, c] = jnp.dot(normed, wq[c], preferred_element_type=f32).astype(bf16)
        if c == 0:
            pl.semaphore_wait(barrier, S - 1 + H - 1)
        for i in range(nch):
            to = partner if i == 0 else xor(chip, i, nch) * 2 + core
            q_copies.append(
                remote(q_all.at[me, c], q_all.at[me, c], q_send.at[i, c], q_recv.at[me, c], seq=to)
            )
            q_copies[-1].start()
        if c == 0:
            def load(i, carry):
                r = device_at(i) if group == 1 else i
                pltpu.make_async_copy(k_hbm.at[r], kbuf.at[r], k_sem.at[r]).start()
                pltpu.make_async_copy(v_hbm.at[r], vbuf.at[r], v_sem.at[r]).start()
                return carry

            lax.fori_loop(0, R, load, 0)
            for h in range(H):
                pltpu.make_async_copy(
                    wo_hbm.at[:, h * W : (h + 1) * W], wo.at[h], wo_sem.at[h]
                ).start()

    slot = me % group
    for which in range(2):
        wkv_copies[which].wait()
        kv_own[slot, which] = jnp.dot(normed, wkv[which], preferred_element_type=f32).astype(bf16)
    base = own_request * group
    kv_copies = []
    for j in range(1, group):
        kv_copies.append(
            remote(
                kv_own.at[slot],
                kv_own.at[slot],
                t_send.at[j],
                t_recv.at[slot],
                seq=base + (slot + j) % group,
            )
        )
        kv_copies[-1].start()
    for j in range(1, group):
        source = (slot + j) % group
        remote(kv_own.at[source], kv_own.at[source], t_send.at[j], t_recv.at[source]).wait_recv()
    for copy in kv_copies:
        copy.wait_send()

    def stacked(block):
        return jnp.concatenate([block[:, g * D : (g + 1) * D] for g in range(G)], axis=0)

    seen = reach_ref[pl.ds(pl.multiple_of(slot * LR, LR), LR), :] > 0.5
    tree_cols = []
    for h in range(KVH):
        keys = jnp.concatenate([kv_own[s, 0, :, h * D : (h + 1) * D] for s in range(group)], axis=0)
        vals = jnp.concatenate([kv_own[s, 1, :, h * D : (h + 1) * D] for s in range(group)], axis=0)
        for g in range(G):
            q = q_all[me, h, :, g * D : (g + 1) * D]
            s = lax.dot_general(q, keys, (((1,), (1,)), ((), ())), preferred_element_type=f32)
            s = jnp.where(seen, s * scale, masked_score)
            m = jnp.max(s, axis=-1, keepdims=True)
            p = jnp.where(seen, jnp.exp(s - m), 0.0)
            total = jnp.maximum(jnp.sum(p, axis=-1, keepdims=True), 1.0)
            o = jnp.dot(p.astype(bf16), vals, preferred_element_type=f32)
            at = (h * G + g) * D
            tree_out[:, at : at + D] = (o / total).astype(bf16)
            tree_cols.append(m + jnp.log(total))
    tree_lse = columns_to_rows(tree_cols, HGP)

    if group > 1:
        for r in range(R):
            pltpu.make_async_copy(k_hbm.at[r], kbuf.at[r], k_sem.at[r]).wait()
            pltpu.make_async_copy(v_hbm.at[r], vbuf.at[r], v_sem.at[r]).wait()

    def attend(i, carry):
        dev = device_at(i)
        r = dev // group

        @pl.when(i > 0)
        def _():
            for c in range(KVH):
                remote(q_all.at[dev, c], q_all.at[dev, c], q_send.at[0, c], q_recv.at[dev, c]).wait_recv()

        @pl.when((i > 0) & (i < nch))
        def _():
            for c in range(KVH):
                block = q_all.at[dev, c]
                remote(block, block, f_send.at[i, c], q_recv.at[dev, c], seq=partner).start()

        if group == 1:
            pltpu.make_async_copy(k_hbm.at[r], kbuf.at[r], k_sem.at[r]).wait()
            pltpu.make_async_copy(v_hbm.at[r], vbuf.at[r], v_sem.at[r]).wait()
        hidden = bias[r]
        cols = []
        for h in range(KVH):
            q = stacked(q_all[dev, h])
            cuts = [slice(at, at + KEYS_AT_ONCE) for at in range(0, LC, KEYS_AT_ONCE)]
            parts = []
            for cut in cuts:
                keys = kbuf[r, cut, h * D : (h + 1) * D]
                s = lax.dot_general(q, keys, (((1,), (1,)), ((), ())), preferred_element_type=f32)
                parts.append(s + hidden[:, cut])
            m = functools.reduce(
                jnp.maximum, [jnp.max(s, axis=-1, keepdims=True) for s in parts]
            )
            total, o = 0.0, 0.0
            for cut, s in zip(cuts, parts):
                p = jnp.exp2((s - m) * exp2_scale)
                total = total + jnp.sum(p, axis=-1, keepdims=True)
                vals = vbuf[r, cut, h * D : (h + 1) * D]
                o = o + jnp.dot(p.astype(bf16), vals, preferred_element_type=f32)
            total = jnp.maximum(total, 1.0)
            o = (o / total).astype(bf16)
            lse = m * scale + jnp.log(total)
            for g in range(G):
                at = (h * G + g) * D
                osend[dev, :, at : at + D] = o[g * LR : (g + 1) * LR]
                cols.append(lse[g * LR : (g + 1) * LR])
        lsend[dev] = columns_to_rows(cols, HGP)

        @pl.when(i > 0)
        def _():
            remote(osend.at[dev], orecv.at[me], o_send.at[i], o_recv.at[me], seq=dev).start()
            remote(lsend.at[dev], lrecv.at[me], l_send.at[i], l_recv.at[me], seq=dev).start()

        return carry

    lax.fori_loop(0, S, attend, 0)

    for copy in q_copies:
        copy.wait_send()
    for i in range(1, nch):
        for c in range(KVH):
            block = q_all.at[me, c]
            remote(block, block, f_send.at[i, c], q_recv.at[me, c]).wait_send()
    orecv[me] = osend[me]
    lrecv[me] = lsend[me]

    def arrive(i, carry):
        dev = device_at(i)
        remote(osend.at[dev], orecv.at[dev], o_send.at[i], o_recv.at[dev]).wait()
        remote(lsend.at[dev], lrecv.at[dev], l_send.at[i], l_recv.at[dev]).wait()
        return carry

    lax.fori_loop(1, S, arrive, 0)

    lse = [lrecv[s] for s in range(S)] + [tree_lse]
    best = functools.reduce(jnp.maximum, lse)
    factors = [jnp.exp(x - best) for x in lse]
    whole = functools.reduce(jnp.add, factors)
    rows = jnp.concatenate([x / whole for x in factors], axis=0)
    pad = -rows.shape[0] % 128
    if pad:
        rows = jnp.concatenate([rows, jnp.zeros((pad, 128), f32)], axis=0)
    weights = rows.T[:LR]
    for n in range(HG):
        at = n * D
        col = S * HGP + n
        total = weights[:, col : col + 1] * tree_out[:, at : at + D].astype(f32)
        for s in range(S):
            col = s * HGP + n
            total = total + weights[:, col : col + 1] * orecv[s, :, at : at + D].astype(f32)
        att[:, at : at + D] = total.astype(bf16)

    for h in range(H):
        pltpu.make_async_copy(wo_hbm.at[:, h * W : (h + 1) * W], wo.at[h], wo_sem.at[h]).wait()
    attended = att[...]
    order = sorted(range(1, H), key=lambda j: -min(j, H - j))
    z_copies = []
    for j in order:
        to = (mh + j) % H
        zsend[j] = jnp.dot(attended, wo[to], preferred_element_type=f32).astype(bf16)
        z_copies.append(
            remote(zsend.at[j], zrecv.at[mh], z_send.at[j], z_recv.at[mh], head=to)
        )
        z_copies[-1].start()
    mixed = jnp.dot(attended, wo[mh], preferred_element_type=f32)
    mixed = mixed + tok[:, pl.ds(pl.multiple_of(mh * W, W), W)].astype(f32)
    for j in order:
        source = (mh + H - j) % H
        remote(zsend.at[j], zrecv.at[source], z_send.at[j], z_recv.at[source]).wait_recv()
        mixed = mixed + zrecv[source].astype(f32)
    out_ref[...] = mixed.astype(bf16)
    for copy in z_copies:
        copy.wait_send()


def solution(mesh):
    S, H = mesh.shape["seq"], mesh.shape["head"]

    def per_device(
        tokens, norm_gain, w_query, key_projection, value_projection, w_out,
        cache_keys, paged_value_cache, lengths, parents, slot_block,
    ):
        LR, M = tokens.shape
        D = HEAD_WIDTH
        KVH = key_projection.shape[1] // D
        G = w_query.shape[1] // key_projection.shape[1]
        R, LC = cache_keys.shape[:2]
        W = w_out.shape[1] // H
        HG = KVH * G
        HGP = -(-HG // 8) * 8
        group = TQ // LR
        dma = pltpu.SemaphoreType.DMA
        vmem = pl.BlockSpec(memory_space=pltpu.VMEM)
        smem = pl.BlockSpec(memory_space=pltpu.SMEM)
        hbm = pl.BlockSpec(memory_space=pl.ANY)
        return pl.pallas_call(
            functools.partial(kernel, (S, H, R, LR, KVH, G, LC)),
            out_shape=jax.ShapeDtypeStruct((LR, W), bf16),
            in_specs=[smem, smem, vmem, vmem] + [hbm] * 7,
            out_specs=vmem,
            scratch_shapes=[
                pltpu.VMEM((LR, M), bf16),
                pltpu.VMEM((KVH, M, G * D), bf16),
                pltpu.VMEM((2, M, KVH * D), bf16),
                pltpu.VMEM((H, HG * D, W), bf16),
                pltpu.VMEM((R, LC, KVH * D), bf16),
                pltpu.VMEM((R, LC, KVH * D), bf16),
                pltpu.VMEM((S, KVH, LR, G * D), bf16),
                pltpu.VMEM((group, 2, LR, KVH * D), bf16),
                pltpu.VMEM((TQ, TQ), f32),
                pltpu.VMEM((R, 1, LC), f32),
                pltpu.VMEM((S, LR, HG * D), bf16),
                pltpu.VMEM((S, LR, HG * D), bf16),
                pltpu.VMEM((S, HGP, 128), f32),
                pltpu.VMEM((S, HGP, 128), f32),
                pltpu.VMEM((LR, HG * D), bf16),
                pltpu.VMEM((LR, HG * D), bf16),
                pltpu.VMEM((H, LR, W), bf16),
                pltpu.VMEM((H, LR, W), bf16),
                dma,
                dma((KVH,)),
                dma((2,)),
                dma((H,)),
                dma((R,)),
                dma((R,)),
                dma((S, KVH)),
                dma((S, KVH)),
                dma((S, KVH)),
                dma((S,)),
                dma((S,)),
                dma((S,)),
                dma((S,)),
                dma((group,)),
                dma((group,)),
                dma((H,)),
                dma((H,)),
            ],
            compiler_params=pltpu.CompilerParams(
                collective_id=0, has_side_effects=True, vmem_limit_bytes=66 * 1000 * 1000
            ),
        )(
            lengths, slot_block, parents, norm_gain, tokens,
            w_query, key_projection, value_projection, w_out, cache_keys, paged_value_cache,
        )

    in_specs = (
        P("seq", None),
        P(),
        P(None, "head"),
        P(None, "head"),
        P(None, "head"),
        P("head", None),
        P(None, "seq", "head"),
        P(None, "seq", "head"),
        P(),
        P(),
        P(None, "seq"),
    )
    return jax.shard_map(
        per_device, mesh=mesh, in_specs=in_specs, out_specs=P("seq", "head"), check_vma=False
    )
```
